32 devices in a mesh: dp: 8 (over z, x), pipe: 2 (over core), tensor: 2 (over y).
Axes of the slice: x: 2, y: 2, z: 4, core: 2. Of those that a mesh axis runs over, the one named last changes fastest.
Arguments:
- hidden: bfloat16 [2, 1024, 3584], P('pipe', 'dp', 'tensor'), may hold values from -6 to 6
- frozen_weight: bfloat16 [3584, 3584], P('dp', 'tensor'), may hold values from -1 to 1
- final_norm_gain: float32 [3584], P('tensor'), may hold values from 0.1 to 1.9
- adapter_down_maps: bfloat16 [8, 32, 3584], P(None, None, 'tensor'), may hold values from -0.09375 to 0.09375
- adapter_up_maps: bfloat16 [8, 32, 3584], P(None, None, 'tensor'), may hold values from -1 to 1
- tenant: int32 [2, 64], P('pipe'), may hold values from 0 to 7, as said below
- adapter: int32 [2], P('pipe'), may hold values from 0 to 7
Outputs:
- upstream_grad: bfloat16 [2, 1024, 3584], P('pipe', 'dp', 'tensor')
- grad_up: float32 [2, 32, 3584], P('pipe', None, 'tensor')
- grad_down: float32 [2, 32, 3584], P('pipe', None, 'tensor')
- row_loss: float32 [2, 64], P('pipe', 'dp')
The draws below stay inside these ranges and needn't reach their ends.
Inputs may be any that keep to these rules, and one draw needn't show every extreme that they name: Rows 2i and 2i + 1 of a micro-batch have the same tenant.
All inputs are finite; a program needn't handle non-finite values.
Results may differ from the reference program's by a relative error of at most 0.024.
Values may be sent and summed in bfloat16 or wider, within the bound.
No kernel may reach another device: no remote copies, remote signals or barrier semaphores. Data moves between devices by JAX's collectives and lax.ppermute only.
A program may use at most 64 MiB of HBM per device.

```python
import jax
import jax.numpy as jnp
from jax import lax

MODEL_WIDTH = 3584
ADAPTER_RANK = 32
ADAPTER_COUNT = 8
SEQ = 16
TENANTS = 8
ROWS_DEV = 8
ROWS = 64
TOKENS = 1024
MICRO = 2
N_DP = 8
N_TENSOR = 2


def draw_tenant(key, part):
    first_key, second_key = jax.random.split(jax.random.fold_in(key, 71))
    first = jax.random.randint(first_key, (MICRO, ROWS // 2), 0, TENANTS)
    second = jax.random.randint(second_key, (MICRO, ROWS // 2), 0, TENANTS)
    paired = jnp.minimum(first, second)
    return jnp.repeat(paired, 2, axis=1).astype(jnp.int32)


def draw_frozen_weight(key, part):
    entry_key, rough_key = jax.random.split(jax.random.fold_in(key, 53))
    level = jnp.arange(MODEL_WIDTH, dtype=jnp.float32) / (MODEL_WIDTH - 1)
    rough = jnp.exp(jax.random.uniform(rough_key, (MODEL_WIDTH,), jnp.float32, -0.4, 0.4))
    column_scale = 10.0 ** level * rough / 4.64
    entries = jax.random.normal(entry_key, (MODEL_WIDTH, MODEL_WIDTH), jnp.float32)
    entries = jnp.clip(entries, -6.0, 6.0) / jnp.sqrt(jnp.float32(MODEL_WIDTH))
    values = jnp.clip(entries * column_scale[None, :], -1.0, 1.0)
    return values.astype(jnp.bfloat16)


def levels(own_key, extent, cuts, low, largest):
    gain = 1.0
    for position, parts in cuts:
        draws = jax.random.uniform(jax.random.fold_in(jax.random.fold_in(own_key, 6), position), (parts,), jnp.float32, low / len(cuts), largest / len(cuts))
        gain = gain * jnp.repeat(jnp.exp(draws), extent[position] // parts).reshape((-1,) + (1,) * (len(extent) - 1 - position))
    return gain


def bell_draw(key, shape, deviation, most, shards=(), held_as=jnp.bfloat16):
    array = deviation * jax.random.normal(key, shape, jnp.float32)
    if shards:
        array = array * levels(key, shape, shards, -0.22, 0.18)
    return jnp.clip(array, -most, most).astype(held_as)


def setup_inputs(seed: int = 0) -> dict:
    arg_keys = jax.random.split(jax.random.key(seed), 8)
    hidden = bell_draw(arg_keys[0], (MICRO, TOKENS, MODEL_WIDTH), 1.0, 6.0, ((0, 2), (1, 8), (2, 2)))
    frozen_weight = draw_frozen_weight(jax.random.fold_in(arg_keys[7], 71), 0)
    final_norm_gain = jnp.clip(1.0 + 0.18 * jax.random.normal(arg_keys[2], (MODEL_WIDTH,), jnp.float32), 0.1, 1.9)
    adapter_down_maps = bell_draw(arg_keys[3], (ADAPTER_COUNT, ADAPTER_RANK, MODEL_WIDTH), MODEL_WIDTH ** -0.5, 0.09375, ((2, 2),))
    adapter_up_maps = bell_draw(arg_keys[4], (ADAPTER_COUNT, ADAPTER_RANK, MODEL_WIDTH), ADAPTER_RANK ** -0.5, 1.0, ((2, 2),))
    tenant = draw_tenant(jax.random.fold_in(arg_keys[7], 71), 0)
    adapter = jax.random.randint(arg_keys[6], (MICRO,), 0, ADAPTER_COUNT).astype(jnp.int32)
    return dict(hidden=hidden, frozen_weight=frozen_weight, final_norm_gain=final_norm_gain, adapter_down_maps=adapter_down_maps, adapter_up_maps=adapter_up_maps, tenant=tenant, adapter=adapter)


logit_divisor = 0.05
loss_scale = 256.0
adapter_scale = 0.5
epsilon = 1e-06

def micro_batch_step(tokens, tenants, down_matrix, up_matrix, frozen_weight, final_norm_gain):
    frozen_output = jnp.dot(tokens, frozen_weight, preferred_element_type=jnp.float32)
    low_rank_hidden = jnp.dot(tokens, down_matrix.T, preferred_element_type=jnp.float32).astype(jnp.bfloat16)
    output_rows = frozen_output + adapter_scale * jnp.dot(low_rank_hidden, up_matrix, preferred_element_type=jnp.float32)
    token_inv = lax.rsqrt(lax.optimization_barrier(jnp.sum(output_rows * output_rows, axis=1)) / MODEL_WIDTH + epsilon)
    normed = output_rows * token_inv[:, None] * final_norm_gain[None, :]
    pooled = lax.optimization_barrier(jnp.mean(normed.reshape(ROWS, SEQ, MODEL_WIDTH), axis=1))
    inverse = lax.rsqrt(lax.optimization_barrier(jnp.sum(pooled * pooled, axis=1)) + epsilon)
    unit_rows = pooled * inverse[:, None]
    encoded_vectors = unit_rows.astype(jnp.bfloat16)
    cosine_logits = jnp.dot(encoded_vectors, encoded_vectors.T, preferred_element_type=jnp.float32) / logit_divisor
    row_ids = jnp.arange(ROWS, dtype=jnp.int32)
    allowed = (tenants[:, None] == tenants[None, :]) & (row_ids[:, None] != row_ids[None, :])
    partner = row_ids[None, :] == (row_ids ^ 1)[:, None]
    exps = jnp.where(allowed, jnp.exp(cosine_logits), 0.0)
    log_total = jnp.log(lax.optimization_barrier(jnp.sum(exps, axis=1)))
    positive = lax.optimization_barrier(jnp.sum(jnp.where(partner, cosine_logits, 0.0), axis=1))
    row_loss = log_total - positive
    probs = jnp.where(allowed, jnp.exp(cosine_logits - log_total[:, None]), 0.0)
    weights = (loss_scale * (probs - partner.astype(jnp.float32))).astype(jnp.bfloat16)
    matching_logits = jnp.dot(weights, encoded_vectors, preferred_element_type=jnp.float32)
    block_weights = weights.reshape(N_DP, ROWS_DEV, ROWS).astype(jnp.float32)
    block_rows = encoded_vectors.reshape(N_DP, ROWS_DEV, MODEL_WIDTH).astype(jnp.float32)
    far_terms = jnp.einsum('kij,kid->kjd', block_weights, block_rows).astype(jnp.bfloat16)
    far_terms = lax.optimization_barrier(far_terms)
    distractor_logits = lax.optimization_barrier(jnp.sum(far_terms.astype(jnp.float32), axis=0))
    encoded_vector_derivative = (matching_logits + distractor_logits) / logit_divisor
    along = lax.optimization_barrier(jnp.sum(unit_rows * encoded_vector_derivative, axis=1))
    grad_pool = inverse[:, None] * (encoded_vector_derivative - unit_rows * along[:, None])
    spread = jnp.broadcast_to((grad_pool * final_norm_gain[None, :])[:, None, :] / SEQ, (ROWS, SEQ, MODEL_WIDTH)).reshape(TOKENS, MODEL_WIDTH)
    inner = lax.optimization_barrier(jnp.sum(spread * output_rows, axis=1))
    grad_norm_in = token_inv[:, None] * (spread - output_rows * (inner * token_inv * token_inv / MODEL_WIDTH)[:, None])
    output_gradient = grad_norm_in.astype(jnp.bfloat16)
    low_rank_gradient = (adapter_scale * jnp.dot(output_gradient, up_matrix.T, preferred_element_type=jnp.float32)).astype(jnp.bfloat16)
    width = MODEL_WIDTH // N_TENSOR
    base_sum = jnp.zeros((TOKENS, MODEL_WIDTH), jnp.float32)
    for block in range(N_TENSOR):
        lower = block * width
        part_sum = jnp.dot(output_gradient[:, lower:lower + width], frozen_weight[:, lower:lower + width].T, preferred_element_type=jnp.float32).astype(jnp.bfloat16)
        part_sum = lax.optimization_barrier(part_sum)
        base_sum = base_sum + part_sum.astype(jnp.float32)
    grad_in = (base_sum + jnp.dot(low_rank_gradient, down_matrix, preferred_element_type=jnp.float32)).astype(jnp.bfloat16)
    up_map_gradient = adapter_scale * jnp.dot(low_rank_hidden.T, output_gradient, preferred_element_type=jnp.float32)
    grad_downward = jnp.dot(low_rank_gradient.T, tokens, preferred_element_type=jnp.float32)
    return (grad_in, up_map_gradient, grad_downward, row_loss)

def reference(hidden, frozen_weight, final_norm_gain, adapter_down_maps, adapter_up_maps, tenant, adapter):
    step_results = []
    for batch_position in range(MICRO):
        picked_adapter = adapter[batch_position]
        step_results.append(micro_batch_step(hidden[batch_position], tenant[batch_position], adapter_down_maps[picked_adapter], adapter_up_maps[picked_adapter], frozen_weight, final_norm_gain))
    grad_in = jnp.stack([item[0] for item in step_results])
    upstream_grad = jnp.roll(grad_in, -1, axis=0)
    grad_up = jnp.stack([item[1] for item in step_results])
    grad_down = jnp.stack([item[2] for item in step_results])
    row_loss = jnp.stack([item[3] for item in step_results])
    return (upstream_grad, grad_up, grad_down, row_loss)
```

```python
import functools

import jax
import jax.numpy as jnp
from jax import lax
from jax.experimental import pallas as pl
from jax.experimental.pallas import tpu as pltpu
from jax.sharding import PartitionSpec as P

MODEL_WIDTH = 3584
SEQ = 16

logit_divisor = 0.05
loss_scale = 256.0
adapter_scale = 0.5
epsilon = 1e-06

F32 = jnp.float32
BF16 = jnp.bfloat16
EXACT = lax.Precision.HIGHEST
LAST = (((1,), (1,)), ((), ()))
FIRST = (((0,), (0,)), ((), ()))


def swapped(block, axis, distance=1, members=None):
    devices = range(lax.axis_size(axis)) if members is None else members
    return lax.ppermute(block, axis, [(i, i ^ distance) for i in devices])


def dot(a, b, dims=(((1,), (0,)), ((), ())), precision=None):
    return lax.dot_general(a, b, dims, precision=precision, preferred_element_type=F32)


def iota(shape, dim):
    return lax.broadcasted_iota(jnp.int32, shape, dim)


def same_sequence(tokens):
    return (iota((tokens, tokens), 0) // SEQ == iota((tokens, tokens), 1) // SEQ).astype(F32)


def column_of(row):
    tokens = row.shape[1]
    eye = iota((tokens, tokens), 0) == iota((tokens, tokens), 1)
    return jnp.sum(jnp.where(eye, row, 0.0), axis=1, keepdims=True)


def spread_rows(rows_local, tokens):
    return (iota((rows_local, tokens), 0) == iota((rows_local, tokens), 1) // SEQ).astype(F32)


def gram_kernel(own_ref, other_ref, gain_ref, up_ref, gram_ref, gained_ref, low_up_ref):
    tokens, half = own_ref.shape
    outputs = jnp.concatenate([own_ref[...], other_ref[...]], axis=1)
    gained = outputs * gain_ref[...]
    gained_ref[...] = gained
    gram = dot(gained, gained, LAST, EXACT) * same_sequence(tokens)
    fold = (iota((SEQ, tokens), 1) % SEQ == iota((SEQ, tokens), 0)).astype(F32)
    gram_ref[0:SEQ, :] = dot(fold, gram, precision=EXACT)
    ones = jnp.ones((8, 2 * half), F32)
    gram_ref[SEQ : SEQ + 8, :] = dot(ones, outputs * outputs, LAST, EXACT)
    low_up_ref[...] = dot(up_ref[...], outputs.astype(BF16), LAST)


def pool_kernel(gram_ref, received_ref, gained_ref, unit_ref, encoded_ref, token_ref):
    tokens = gained_ref.shape[0]
    rows_local = tokens // SEQ
    total = gram_ref[...] + received_ref[...]
    token_inv = lax.rsqrt(total[SEQ : SEQ + 1, :] / MODEL_WIDTH + epsilon)
    same = same_sequence(tokens)
    place = (iota((SEQ, tokens), 1) % SEQ == iota((SEQ, tokens), 0)).astype(F32)
    peers = dot(place * token_inv, same, precision=EXACT)
    weighted = jnp.sum(total[0:SEQ, :] * peers, axis=0, keepdims=True)
    parts = jnp.broadcast_to(token_inv * weighted, (8, tokens))
    squares = dot(parts, same, precision=EXACT)[0:1, :] / (SEQ * SEQ)
    inverse = lax.rsqrt(squares + epsilon)
    pick = spread_rows(rows_local, tokens) * (token_inv * inverse / SEQ)
    unit = dot(pick, gained_ref[...], precision=EXACT)
    unit_ref[...] = unit
    encoded_ref[...] = unit.astype(BF16)
    token_ref[0:1, :] = token_inv
    token_ref[1:2, :] = inverse
    token_ref[2:3, :] = inverse * weighted / SEQ
    token_ref[3:8, :] = jnp.zeros((5, tokens), F32)


def score_kernel(rows_ref, gained_ref, gain_ref, up_ref, low_up_ref, out_ref):
    total_rows = rows_ref.shape[0]
    rank, tokens = low_up_ref.shape
    width = out_ref.shape[1]

    def put(start, value):
        rows, columns = value.shape
        if columns < width:
            value = jnp.concatenate([value, jnp.zeros((rows, width - columns), F32)], axis=1)
        out_ref[start : start + rows, :] = value

    rows = rows_ref[...]
    gained_rows = (rows.astype(F32) * gain_ref[...]).astype(BF16)
    put(0, dot(rows, rows, LAST))
    put(total_rows, dot(rows, gained_ref[...].astype(BF16), LAST))
    put(2 * total_rows, low_up_ref[...])
    put(2 * total_rows + rank, dot(up_ref[...], gained_rows, LAST))


def loss_kernel(
    part_ref,
    received_ref,
    tenant_row_ref,
    tenant_column_ref,
    token_ref,
    rows_ref,
    unit_ref,
    own_ref,
    other_ref,
    gain_ref,
    low_ref,
    hidden_ref,
    loss_ref,
    adapter_ref,
    spread_ref,
    late_ref,
):
    total_rows = rows_ref.shape[0]
    rows_local = unit_ref.shape[0]
    rank, tokens = low_ref.shape
    total = part_ref[...] + received_ref[...]
    products = total[0:total_rows, 0:total_rows]
    scores = products / logit_divisor
    from_row = iota((total_rows, total_rows), 0)
    from_column = iota((total_rows, total_rows), 1)
    allowed = (tenant_row_ref[...] == tenant_column_ref[...]) & (from_row != from_column)
    partner = from_column == (from_row ^ 1)
    exps = jnp.where(allowed, jnp.exp(scores), 0.0)
    log_total = jnp.log(jnp.sum(exps, axis=1, keepdims=True))
    positive = jnp.sum(jnp.where(partner, scores, 0.0), axis=1, keepdims=True)
    own = (iota((total_rows, rows_local), 0) == iota((total_rows, rows_local), 1)).astype(F32)
    loss_ref[...] = jnp.sum((log_total - positive) * own, axis=0, keepdims=True)
    probs = jnp.where(allowed, jnp.exp(scores - log_total), 0.0)
    weights = loss_scale * (probs - partner.astype(F32))
    weights = weights.astype(BF16)
    near = weights[0:rows_local, :]
    far = dot(own.astype(BF16), weights, (((0,), (1,)), ((), ()))).astype(BF16)
    both = near.astype(F32) + far.astype(F32)
    rows = rows_ref[...]
    derivative = (dot(near, rows) + dot(far, rows)) / logit_divisor
    along = jnp.sum(both * products[0:rows_local, :], axis=1, keepdims=True) / logit_divisor
    expand = spread_rows(rows_local, tokens)
    along_row = jnp.sum(along * expand, axis=0, keepdims=True)
    token_weights = dot(both, expand, FIRST, EXACT)
    first = jnp.sum(token_weights * total[total_rows : 2 * total_rows, 0:tokens], axis=0, keepdims=True)
    first = first / logit_divisor
    token_inv = token_ref[0:1, :]
    inverse = token_ref[1:2, :]
    second = token_ref[2:3, :]
    inner = inverse * (first - along_row * second) / SEQ
    decay = token_inv * token_inv * token_inv * inner / MODEL_WIDTH
    inverse_column = jnp.sum(expand * inverse, axis=1, keepdims=True) / SEQ
    unit = unit_ref[...]
    spread = inverse_column * (derivative - unit * along) * gain_ref[...] / SEQ
    spread_ref[...] = spread
    inv_column = column_of(token_inv)
    decay_column = column_of(decay)
    half = own_ref.shape[1]
    width = 2 * half
    wide = jnp.broadcast_to(spread[:, None, :], (rows_local, SEQ, width)).reshape(tokens, width)
    outputs = jnp.concatenate([own_ref[...], other_ref[...]], axis=1)
    output_gradient = (inv_column * wide - decay_column * outputs).astype(BF16)
    adapter_ref[0:rank, :] = (adapter_scale * dot(low_ref[...], output_gradient)).astype(BF16)
    start = 2 * total_rows
    low_up = total[start : start + rank, 0:tokens]
    rows_up = total[start + rank : start + 2 * rank, 0:total_rows]
    sums_up = dot(rows_up, token_weights, precision=EXACT) / logit_divisor
    own_up = dot(rows_up[:, 0:rows_local], expand, precision=EXACT)
    spread_up = inverse * (sums_up - own_up * along_row) / SEQ
    low_gradient = (adapter_scale * (token_inv * spread_up - decay * low_up)).astype(BF16)
    adapter_ref[rank : 2 * rank, :] = dot(low_gradient, hidden_ref[...]).astype(BF16)
    late_ref[0:rank, :] = low_gradient.astype(F32)
    late_ref[rank : rank + 1, :] = token_inv
    late_ref[rank + 1 : rank + 2, :] = decay
    late_ref[rank + 2 : rank + 8, :] = jnp.zeros((6, tokens), F32)


def input_kernel(late_ref, spread_ref, part_ref, received_ref, down_ref, out_ref):
    tokens, width = part_ref.shape
    rank = down_ref.shape[0]
    rows_local = spread_ref.shape[0]
    inv_column = column_of(late_ref[rank : rank + 1, :])
    decay_column = column_of(late_ref[rank + 1 : rank + 2, :])
    low_gradient = late_ref[0:rank, :].astype(BF16)
    wide = jnp.broadcast_to(spread_ref[...][:, None, :], (rows_local, SEQ, width))
    total = part_ref[...] + received_ref[...].astype(F32)
    base = inv_column * wide.reshape(tokens, width) - decay_column * total
    out_ref[...] = (base + dot(low_gradient, down_ref[...], FIRST)).astype(BF16)


def call(kernel, outs, *args):
    vmem = pl.BlockSpec(memory_space=pltpu.VMEM)
    size = sum(a.size * a.dtype.itemsize for a in args)
    return pl.pallas_call(
        kernel,
        out_shape=[jax.ShapeDtypeStruct(shape, dtype) for shape, dtype in outs],
        in_specs=[vmem] * len(args),
        out_specs=[vmem] * len(outs),
        cost_estimate=pl.CostEstimate(flops=2**28, bytes_accessed=size, transcendentals=0),
        compiler_params=pltpu.CompilerParams(vmem_limit_bytes=32 * 2**20),
    )(*args)


def gathered_weight(own):
    count = lax.axis_size("dp")
    block, columns = own.shape
    position = lax.axis_index("dp")
    if count == 8:
        line = position // 2
        is_inner = (line == 1) | (line == 2)
        inner = [i for i in range(count) if i // 2 in (1, 2)]
        outer = [i for i in range(count) if i // 2 in (0, 3)]
        forward = [(i ^ 2, i) for i in outer]
        across = swapped(own, "dp", 6, inner)
        near = swapped(own, "dp", 2)
        own_x = swapped(own, "dp", 1)
        forward_first = lax.ppermute(across, "dp", forward)
        across_second = swapped(near, "dp", 6, inner)
        near_x = swapped(near, "dp", 1)
        forward_second = lax.ppermute(across_second, "dp", forward)
        second = jnp.where(is_inner, across_second, forward_first)
        third = jnp.where(is_inner, across, forward_second)
        second_x = swapped(second, "dp", 1)
        third_x = jnp.where(
            is_inner, swapped(across, "dp", 1, inner), swapped(forward_second, "dp", 1, outer)
        )
        slots = (own, own_x, near, near_x, second, second_x, third, third_x)
    else:
        slots = (own,)
        held = own
        distance = 1
        while distance < count:
            held = jnp.concatenate([held, swapped(held, "dp", distance)], axis=0)
            distance *= 2
        slots = tuple(held[i * block : (i + 1) * block] for i in range(count))
    whole = jnp.zeros((count * block, columns), own.dtype)
    for i, slot in enumerate(slots):
        whole = lax.dynamic_update_slice(whole, slot, ((position ^ i) * block, 0))
    return whole


def body(
    hidden, frozen_weight, final_norm_gain, adapter_down_maps, adapter_up_maps, tenant, adapter
):
    own_tokens = hidden[0]
    tokens, half_width = own_tokens.shape
    rows_local = tokens // SEQ
    columns = half_width // 2
    rank = adapter_up_maps.shape[1]
    count = lax.axis_size("dp")
    position = lax.axis_index("dp")
    side = lax.axis_index("tensor")
    core = lax.axis_index("pipe") & 1
    crossed = lax.axis_size("pipe") == 2
    total_rows = count * rows_local

    weight_part = lax.dynamic_slice_in_dim(frozen_weight, core * columns, columns, axis=1)
    weight = gathered_weight(weight_part)

    received_tokens = swapped(own_tokens, "tensor")
    full_tokens = jnp.where(
        side == 0,
        jnp.concatenate([own_tokens, received_tokens], axis=1),
        jnp.concatenate([received_tokens, own_tokens], axis=1),
    )
    other_tokens = swapped(full_tokens, "pipe")
    picked = adapter[0]
    other_picked = swapped(adapter, "pipe")[0]
    pick = functools.partial(lax.dynamic_index_in_dim, axis=0, keepdims=False)
    down_matrix = pick(adapter_down_maps, picked)
    up_matrix = pick(adapter_up_maps, picked)
    other_up = pick(adapter_up_maps, other_picked)
    low_part = dot(down_matrix, own_tokens, LAST)
    low = (low_part + swapped(low_part, "tensor")).astype(BF16)
    other_low = swapped(low, "pipe")
    up_columns = lax.dynamic_slice_in_dim(up_matrix, core * columns, columns, axis=1)
    other_up_columns = lax.dynamic_slice_in_dim(other_up, core * columns, columns, axis=1)

    both_tokens = jnp.concatenate([full_tokens, other_tokens], axis=0)
    low_outputs = jnp.concatenate(
        [dot(low, up_columns, FIRST), dot(other_low, other_up_columns, FIRST)], axis=0
    )
    outputs = dot(both_tokens, weight) + adapter_scale * low_outputs

    own_outputs = outputs[:tokens]
    other_outputs = swapped(outputs[tokens:], "pipe")

    def own_first(array):
        lower, upper = array[..., :columns], array[..., columns:]
        return jnp.where(
            core == 0,
            jnp.concatenate([lower, upper], axis=-1),
            jnp.concatenate([upper, lower], axis=-1),
        )

    gain = own_first(final_norm_gain[None, :])
    up_ordered = own_first(up_matrix)

    product = dot(outputs.astype(BF16), weight, LAST)
    kept, sent = (product[tokens:], product[:tokens])
    if not crossed:
        kept, sent = sent, kept
    reduced = kept + swapped(sent.astype(BF16), "pipe").astype(F32)
    far_half = lax.dynamic_slice_in_dim(reduced, (1 - side) * half_width, half_width, axis=1)
    near_half = lax.dynamic_slice_in_dim(reduced, side * half_width, half_width, axis=1)
    received_half = swapped(far_half.astype(BF16), "tensor")

    gram, gained, low_up = call(
        gram_kernel,
        [((SEQ + 8, tokens), F32), ((tokens, half_width), F32), ((rank, tokens), F32)],
        own_outputs,
        other_outputs,
        gain,
        up_ordered,
    )
    received_gram = swapped(gram, "tensor")
    unit, encoded, token_terms = call(
        pool_kernel,
        [((rows_local, half_width), F32), ((rows_local, half_width), BF16), ((8, tokens), F32)],
        gram,
        received_gram,
        gained,
    )
    all_rows = encoded
    distance = 1
    while distance < count:
        all_rows = jnp.concatenate([all_rows, swapped(all_rows, "dp", distance)], axis=0)
        distance *= 2
    (score_part,) = call(
        score_kernel,
        [((2 * total_rows + 2 * rank, max(tokens, total_rows)), F32)],
        all_rows,
        gained,
        gain,
        up_ordered,
        low_up,
    )
    received_scores = swapped(score_part, "tensor")

    place = jnp.arange(total_rows, dtype=jnp.int32)
    row_ids = ((place // rows_local) ^ position) * rows_local + place % rows_local
    chosen = (row_ids[:, None] == place[None, :]) * tenant[0][None, :]
    tenants = jnp.sum(chosen, axis=1)
    row_loss, adapter_part, spread, late = call(
        loss_kernel,
        [
            ((1, rows_local), F32),
            ((2 * rank, half_width), BF16),
            ((rows_local, half_width), F32),
            ((rank + 8, tokens), F32),
        ],
        score_part,
        received_scores,
        tenants[None, :],
        tenants[:, None],
        token_terms,
        all_rows,
        unit,
        own_outputs,
        other_outputs,
        gain,
        low,
        own_tokens,
    )

    adapter_sum = adapter_part
    distance = 1
    while distance < count:
        received = swapped(adapter_sum, "dp", distance)
        adapter_sum = adapter_sum.astype(F32) + received.astype(F32)
        distance *= 2
        if distance < count:
            adapter_sum = adapter_sum.astype(BF16)
    up_gradient = own_first(adapter_sum[:rank])
    down_gradient = adapter_sum[rank:]

    other_spread = swapped(spread[:, columns:], "pipe")
    spreads = jnp.concatenate([spread[:, :columns], other_spread], axis=0).astype(BF16)
    spread_product = dot(spreads, weight, LAST)
    kept, sent = (spread_product[rows_local:], spread_product[:rows_local])
    if not crossed:
        kept, sent = sent, kept
    spread_sum = kept + swapped(sent, "pipe")
    spread_far = lax.dynamic_slice_in_dim(spread_sum, (1 - side) * half_width, half_width, axis=1)
    spread_near = lax.dynamic_slice_in_dim(spread_sum, side * half_width, half_width, axis=1)
    spread_total = spread_near + swapped(spread_far, "tensor")
    if crossed:
        late = swapped(late, "pipe")
        down_matrix = pick(adapter_down_maps, other_picked)
    (handed,) = call(
        input_kernel,
        [((tokens, half_width), BF16)],
        late,
        spread_total,
        near_half,
        received_half,
        down_matrix,
    )
    if not crossed:
        members = range(lax.axis_size("pipe"))
        handed = lax.ppermute(handed, "pipe", [((i + 1) % len(members), i) for i in members])
    return (handed[None], up_gradient[None], down_gradient[None], row_loss)


def solution(mesh):
    return jax.shard_map(
        body,
        mesh=mesh,
        in_specs=(
            P("pipe", "dp", "tensor"),
            P("dp", "tensor"),
            P("tensor"),
            P(None, None, "tensor"),
            P(None, None, "tensor"),
            P("pipe", None),
            P("pipe"),
        ),
        out_specs=(
            P("pipe", "dp", "tensor"),
            P("pipe", None, "tensor"),
            P("pipe", None, "tensor"),
            P("pipe", "dp"),
        ),
        check_vma=False,
    )
```

```python
import functools

import jax
import jax.numpy as jnp
from jax import lax
from jax.experimental import pallas as pl
from jax.experimental.pallas import tpu as pltpu
from jax.sharding import PartitionSpec as P

MODEL_WIDTH = 3584
SEQ = 16

logit_divisor = 0.05
loss_scale = 256.0
adapter_scale = 0.5
epsilon = 1e-06

F32 = jnp.float32
BF16 = jnp.bfloat16
EXACT = lax.Precision.HIGHEST
LAST = (((1,), (1,)), ((), ()))
FIRST = (((0,), (0,)), ((), ()))

CHUNKS = 2


def swapped(block, axis, distance=1, members=None):
    devices = range(lax.axis_size(axis)) if members is None else members
    return lax.ppermute(block, axis, [(i, i ^ distance) for i in devices])


def dot(a, b, dims=(((1,), (0,)), ((), ())), precision=None):
    return lax.dot_general(a, b, dims, precision=precision, preferred_element_type=F32)


def iota(shape, dim):
    return lax.broadcasted_iota(jnp.int32, shape, dim)


def same_sequence(tokens):
    return (iota((tokens, tokens), 0) // SEQ == iota((tokens, tokens), 1) // SEQ).astype(F32)


def column_of(row):
    tokens = row.shape[1]
    eye = iota((tokens, tokens), 0) == iota((tokens, tokens), 1)
    return jnp.sum(jnp.where(eye, row, 0.0), axis=1, keepdims=True)


def spread_rows(rows_local, tokens):
    return (iota((rows_local, tokens), 0) == iota((rows_local, tokens), 1) // SEQ).astype(F32)


def gram_kernel(own_ref, other_ref, gain_ref, up_ref, gram_ref, gained_ref, low_up_ref):
    tokens, half = own_ref.shape
    outputs = jnp.concatenate([own_ref[...], other_ref[...]], axis=1)
    gained = outputs * gain_ref[...]
    gained_ref[...] = gained
    gram = dot(gained, gained, LAST, EXACT) * same_sequence(tokens)
    fold = (iota((SEQ, tokens), 1) % SEQ == iota((SEQ, tokens), 0)).astype(F32)
    gram_ref[0:SEQ, :] = dot(fold, gram, precision=EXACT)
    ones = jnp.ones((8, 2 * half), F32)
    gram_ref[SEQ : SEQ + 8, :] = dot(ones, outputs * outputs, LAST, EXACT)
    low_up_ref[...] = dot(up_ref[...], outputs.astype(BF16), LAST)


def pool_kernel(gram_ref, received_ref, gained_ref, unit_ref, encoded_ref, token_ref):
    tokens = gained_ref.shape[0]
    rows_local = tokens // SEQ
    total = gram_ref[...] + received_ref[...]
    token_inv = lax.rsqrt(total[SEQ : SEQ + 1, :] / MODEL_WIDTH + epsilon)
    same = same_sequence(tokens)
    place = (iota((SEQ, tokens), 1) % SEQ == iota((SEQ, tokens), 0)).astype(F32)
    peers = dot(place * token_inv, same, precision=EXACT)
    weighted = jnp.sum(total[0:SEQ, :] * peers, axis=0, keepdims=True)
    parts = jnp.broadcast_to(token_inv * weighted, (8, tokens))
    squares = dot(parts, same, precision=EXACT)[0:1, :] / (SEQ * SEQ)
    inverse = lax.rsqrt(squares + epsilon)
    pick = spread_rows(rows_local, tokens) * (token_inv * inverse / SEQ)
    unit = dot(pick, gained_ref[...], precision=EXACT)
    unit_ref[...] = unit
    encoded_ref[...] = unit.astype(BF16)
    token_ref[0:1, :] = token_inv
    token_ref[1:2, :] = inverse
    token_ref[2:3, :] = inverse * weighted / SEQ
    token_ref[3:8, :] = jnp.zeros((5, tokens), F32)


def score_kernel(rows_ref, gained_ref, gain_ref, up_ref, low_up_ref, out_ref):
    total_rows = rows_ref.shape[0]
    rank, tokens = low_up_ref.shape
    width = out_ref.shape[1]

    def put(start, value):
        rows, columns = value.shape
        if columns < width:
            value = jnp.concatenate([value, jnp.zeros((rows, width - columns), F32)], axis=1)
        out_ref[start : start + rows, :] = value

    rows = rows_ref[...]
    gained_rows = (rows.astype(F32) * gain_ref[...]).astype(BF16)
    put(0, dot(rows, rows, LAST))
    put(total_rows, dot(rows, gained_ref[...].astype(BF16), LAST))
    put(2 * total_rows, low_up_ref[...])
    put(2 * total_rows + rank, dot(up_ref[...], gained_rows, LAST))


def loss_kernel(
    part_ref,
    received_ref,
    tenant_row_ref,
    tenant_column_ref,
    token_ref,
    rows_ref,
    unit_ref,
    own_ref,
    other_ref,
    gain_ref,
    low_ref,
    hidden_ref,
    loss_ref,
    adapter_ref,
    spread_ref,
    late_ref,
):
    total_rows = rows_ref.shape[0]
    rows_local = unit_ref.shape[0]
    rank, tokens = low_ref.shape
    total = part_ref[...] + received_ref[...]
    products = total[0:total_rows, 0:total_rows]
    scores = products / logit_divisor
    from_row = iota((total_rows, total_rows), 0)
    from_column = iota((total_rows, total_rows), 1)
    allowed = (tenant_row_ref[...] == tenant_column_ref[...]) & (from_row != from_column)
    partner = from_column == (from_row ^ 1)
    exps = jnp.where(allowed, jnp.exp(scores), 0.0)
    log_total = jnp.log(jnp.sum(exps, axis=1, keepdims=True))
    positive = jnp.sum(jnp.where(partner, scores, 0.0), axis=1, keepdims=True)
    own = (iota((total_rows, rows_local), 0) == iota((total_rows, rows_local), 1)).astype(F32)
    loss_ref[...] = jnp.sum((log_total - positive) * own, axis=0, keepdims=True)
    probs = jnp.where(allowed, jnp.exp(scores - log_total), 0.0)
    weights = loss_scale * (probs - partner.astype(F32))
    weights = weights.astype(BF16)
    near = weights[0:rows_local, :]
    far = dot(own.astype(BF16), weights, (((0,), (1,)), ((), ()))).astype(BF16)
    both = near.astype(F32) + far.astype(F32)
    rows = rows_ref[...]
    derivative = (dot(near, rows) + dot(far, rows)) / logit_divisor
    along = jnp.sum(both * products[0:rows_local, :], axis=1, keepdims=True) / logit_divisor
    expand = spread_rows(rows_local, tokens)
    along_row = jnp.sum(along * expand, axis=0, keepdims=True)
    token_weights = dot(both, expand, FIRST, EXACT)
    first = jnp.sum(token_weights * total[total_rows : 2 * total_rows, 0:tokens], axis=0, keepdims=True)
    first = first / logit_divisor
    token_inv = token_ref[0:1, :]
    inverse = token_ref[1:2, :]
    second = token_ref[2:3, :]
    inner = inverse * (first - along_row * second) / SEQ
    decay = token_inv * token_inv * token_inv * inner / MODEL_WIDTH
    inverse_column = jnp.sum(expand * inverse, axis=1, keepdims=True) / SEQ
    unit = unit_ref[...]
    spread = inverse_column * (derivative - unit * along) * gain_ref[...] / SEQ
    spread_ref[...] = spread
    inv_column = column_of(token_inv)
    decay_column = column_of(decay)
    half = own_ref.shape[1]
    width = 2 * half
    wide = jnp.broadcast_to(spread[:, None, :], (rows_local, SEQ, width)).reshape(tokens, width)
    outputs = jnp.concatenate([own_ref[...], other_ref[...]], axis=1)
    output_gradient = (inv_column * wide - decay_column * outputs).astype(BF16)
    adapter_ref[0:rank, :] = (adapter_scale * dot(low_ref[...], output_gradient)).astype(BF16)
    start = 2 * total_rows
    low_up = total[start : start + rank, 0:tokens]
    rows_up = total[start + rank : start + 2 * rank, 0:total_rows]
    sums_up = dot(rows_up, token_weights, precision=EXACT) / logit_divisor
    own_up = dot(rows_up[:, 0:rows_local], expand, precision=EXACT)
    spread_up = inverse * (sums_up - own_up * along_row) / SEQ
    low_gradient = (adapter_scale * (token_inv * spread_up - decay * low_up)).astype(BF16)
    adapter_ref[rank : 2 * rank, :] = dot(low_gradient, hidden_ref[...]).astype(BF16)
    late_ref[0:rank, :] = low_gradient.astype(F32)
    late_ref[rank : rank + 1, :] = token_inv
    late_ref[rank + 1 : rank + 2, :] = decay
    late_ref[rank + 2 : rank + 8, :] = jnp.zeros((6, tokens), F32)


def input_kernel(late_ref, spread_ref, part_ref, received_ref, down_ref, out_ref):
    tokens, width = part_ref.shape
    rank = down_ref.shape[0]
    rows_local = spread_ref.shape[0]
    inv_column = column_of(late_ref[rank : rank + 1, :])
    decay_column = column_of(late_ref[rank + 1 : rank + 2, :])
    low_gradient = late_ref[0:rank, :].astype(BF16)
    wide = jnp.broadcast_to(spread_ref[...][:, None, :], (rows_local, SEQ, width))
    total = part_ref[...] + received_ref[...].astype(F32)
    base = inv_column * wide.reshape(tokens, width) - decay_column * total
    out_ref[...] = (base + dot(low_gradient, down_ref[...], FIRST)).astype(BF16)


def call(kernel, outs, *args):
    vmem = pl.BlockSpec(memory_space=pltpu.VMEM)
    size = sum(a.size * a.dtype.itemsize for a in args)
    return pl.pallas_call(
        kernel,
        out_shape=[jax.ShapeDtypeStruct(shape, dtype) for shape, dtype in outs],
        in_specs=[vmem] * len(args),
        out_specs=[vmem] * len(outs),
        cost_estimate=pl.CostEstimate(flops=2**28, bytes_accessed=size, transcendentals=0),
        compiler_params=pltpu.CompilerParams(vmem_limit_bytes=40 * 2**20),
    )(*args)


def distances(count):
    return [2**i for i in range(count.bit_length() - 1)]


def gathered_blocks(own):
    count = lax.axis_size("dp")
    if count != 8:
        block = own.shape[0]
        held = own
        for distance in distances(count):
            held = jnp.concatenate([held, swapped(held, "dp", distance)], axis=0)
        return [[held[i * block : (i + 1) * block]] for i in range(count)]
    line = lax.axis_index("dp") // 2
    is_inner = (line == 1) | (line == 2)
    inner = [i for i in range(count) if i // 2 in (1, 2)]
    outer = [i for i in range(count) if i // 2 in (0, 3)]
    forward = [(i ^ 2, i) for i in outer]
    rows = own.shape[0] // CHUNKS
    states = [dict(own=own[i * rows : (i + 1) * rows]) for i in range(CHUNKS)]
    results = []
    for step in range(4 * CHUNKS):
        state = states[step % CHUNKS]
        if step >= 2:
            earlier = results[step - 2]
            tied = lax.optimization_barrier({**state, **earlier})
            states[(step - 2) % CHUNKS].update({name: tied[name] for name in earlier})
            state.update({name: tied[name] for name in state})
        stage = step // CHUNKS
        if stage == 0:
            new = dict(
                near=swapped(state["own"], "dp", 2),
                across=swapped(state["own"], "dp", 6, inner),
                own_x=swapped(state["own"], "dp", 1),
            )
        elif stage == 1:
            new = dict(
                across_second=swapped(state["near"], "dp", 6, inner),
                forward_first=lax.ppermute(state["across"], "dp", forward),
                near_x=swapped(state["near"], "dp", 1),
            )
        elif stage == 2:
            second = jnp.where(is_inner, state["across_second"], state["forward_first"])
            state["second"] = lax.optimization_barrier(second)
            new = dict(
                forward_second=lax.ppermute(state["across_second"], "dp", forward),
                second_x=swapped(state["second"], "dp", 1),
            )
        else:
            third = jnp.where(is_inner, state["across"], state["forward_second"])
            state["third"] = lax.optimization_barrier(third)
            new = dict(third_x=swapped(state["third"], "dp", 1))
        state.update(new)
        results.append(new)
    names = ("own", "own_x", "near", "near_x", "second", "second_x", "third", "third_x")
    return [[state[name] for state in states] for name in names]


def forward_kernel(first, chunks, *refs):
    own_ref, other_ref, start_ref = refs[:3]
    count = (len(refs) - 3 - (2 if first else 4)) // chunks
    pieces, outs = refs[3 : 3 + count * chunks], refs[3 + count * chunks :]
    total_ref, weight_ref = outs[0], outs[-1]
    position = lax.axis_index("dp")
    rows, columns = pieces[0].shape
    block = rows * chunks
    tokens = own_ref.shape[0]
    total = start_ref[...]
    offset = 0 if first else own_ref.shape[1] // (2 * block) - count // 2
    for pair in range(count // 2):
        for i in range(2):
            where = pair * 2 * block + ((position & 1) ^ i) * block
            for j in range(chunks):
                place = pl.ds(pl.multiple_of(where + j * rows, 16), rows)
                weight_ref[place, :] = pieces[(2 * pair + i) * chunks + j][...]
        lane = pl.ds(pl.multiple_of(((position >> 1) ^ (pair + offset)) * 2 * block, 128), 2 * block)
        x = jnp.concatenate([own_ref[:, lane], other_ref[:, lane]], axis=0)
        total = total + dot(x, weight_ref[pair * 2 * block : (pair + 1) * 2 * block, :])
    if first:
        total_ref[...] = total
    else:
        total_ref[...] = total[:tokens]
        outs[1][...] = total[tokens:]
        outs[2][...] = total.astype(BF16)


def product_kernel(rows_ref, low_ref, high_ref, near_ref, far_ref):
    size = rows_ref.shape[1]
    rows = rows_ref[...].astype(BF16)
    bit = (lax.axis_index("dp") >> 1) & 1
    for i in range(2):
        weight = low_ref[pl.ds(pl.multiple_of((bit ^ i) * size, 128), size), :]
        near_ref[:, i * size : (i + 1) * size] = dot(rows, weight, LAST)
        weight = jnp.where(bit == i, low_ref[2 * size : 3 * size, :], high_ref[...])
        far_ref[:, i * size : (i + 1) * size] = dot(rows, weight, LAST)


def body(
    hidden, frozen_weight, final_norm_gain, adapter_down_maps, adapter_up_maps, tenant, adapter
):
    own_tokens = hidden[0]
    tokens, half_width = own_tokens.shape
    rows_local = tokens // SEQ
    columns = half_width // 2
    rank = adapter_up_maps.shape[1]
    count = lax.axis_size("dp")
    position = lax.axis_index("dp")
    side = lax.axis_index("tensor")
    core = lax.axis_index("pipe") & 1
    crossed = lax.axis_size("pipe") == 2
    total_rows = count * rows_local

    weight_part = lax.dynamic_slice_in_dim(frozen_weight, core * columns, columns, axis=1)
    slots = gathered_blocks(weight_part)
    received_tokens = swapped(own_tokens, "tensor")
    full_tokens = jnp.where(
        side == 0,
        jnp.concatenate([own_tokens, received_tokens], axis=1),
        jnp.concatenate([received_tokens, own_tokens], axis=1),
    )
    other_tokens = swapped(full_tokens, "pipe")
    picked = adapter[0]
    other_picked = swapped(adapter, "pipe")[0]
    pick = functools.partial(lax.dynamic_index_in_dim, axis=0, keepdims=False)
    down_matrix = pick(adapter_down_maps, picked)
    up_matrix = pick(adapter_up_maps, picked)
    other_up = pick(adapter_up_maps, other_picked)
    low_part = dot(down_matrix, own_tokens, LAST)
    low = (low_part + swapped(low_part, "tensor")).astype(BF16)
    other_low = swapped(low, "pipe")
    up_columns = lax.dynamic_slice_in_dim(up_matrix, core * columns, columns, axis=1)
    other_up_columns = lax.dynamic_slice_in_dim(other_up, core * columns, columns, axis=1)

    low_outputs = adapter_scale * jnp.concatenate(
        [dot(low, up_columns, FIRST), dot(other_low, other_up_columns, FIRST)], axis=0
    )
    in_pairs = count == 8 and (2 * weight_part.shape[0]) % 128 == 0
    if in_pairs:
        early = [piece for slot in slots[:6] for piece in slot]
        last = [piece for slot in slots[6:] for piece in slot]
        pair_rows = 2 * weight_part.shape[0]
        partial_outputs, weight_low = call(
            functools.partial(forward_kernel, True, len(slots[0])),
            [((2 * tokens, columns), F32), ((3 * pair_rows, columns), BF16)],
            full_tokens,
            other_tokens,
            low_outputs,
            *early,
        )
        own_outputs, sent_outputs, outputs_low, weight_high = call(
            functools.partial(forward_kernel, False, len(slots[0])),
            [
                ((tokens, columns), F32),
                ((tokens, columns), F32),
                ((2 * tokens, columns), BF16),
                ((pair_rows, columns), BF16),
            ],
            full_tokens,
            other_tokens,
            partial_outputs,
            *last,
        )
        is_lower = (position >> 2) == side
    else:
        weight = jnp.zeros((count * weight_part.shape[0], columns), BF16)
        for i, (piece,) in enumerate(slots):
            start = (position ^ i) * weight_part.shape[0]
            weight = lax.dynamic_update_slice(weight, piece, (start, 0))
        both_tokens = jnp.concatenate([full_tokens, other_tokens], axis=0)
        outputs = dot(both_tokens, weight) + low_outputs
        own_outputs, sent_outputs = outputs[:tokens], outputs[tokens:]
        outputs_low = outputs.astype(BF16)
        is_lower = side == 0

    def features(rows, name):
        with jax.named_scope(name):
            if in_pairs:
                shape = (rows.shape[0], half_width)
                products = call(
                    product_kernel, [(shape, F32)] * 2, rows, weight_low, weight_high
                )
            else:
                product = dot(rows.astype(BF16), weight, LAST)
                products = (product[:, :half_width], product[:, half_width:])
        sums = []
        half = rows.shape[0] // 2
        for product in products:
            kept, sent = (product[half:], product[:half])
            if not crossed:
                kept, sent = sent, kept
            if half == tokens:
                sent = sent.astype(BF16)
            sums.append(kept + swapped(sent, "pipe").astype(F32))
        lower, upper = sums
        return jnp.where(is_lower, lower, upper), jnp.where(is_lower, upper, lower)

    other_outputs = swapped(sent_outputs, "pipe")

    def own_first(array):
        lower, upper = array[..., :columns], array[..., columns:]
        return jnp.where(
            core == 0,
            jnp.concatenate([lower, upper], axis=-1),
            jnp.concatenate([upper, lower], axis=-1),
        )

    gain = own_first(final_norm_gain[None, :])
    up_ordered = own_first(up_matrix)

    near_half, far_half = features(outputs_low, "early")
    received_half = swapped(far_half.astype(BF16), "tensor")

    gram, gained, low_up = call(
        gram_kernel,
        [((SEQ + 8, tokens), F32), ((tokens, half_width), F32), ((rank, tokens), F32)],
        own_outputs,
        other_outputs,
        gain,
        up_ordered,
    )
    received_gram = swapped(gram, "tensor")
    unit, encoded, token_terms = call(
        pool_kernel,
        [((rows_local, half_width), F32), ((rows_local, half_width), BF16), ((8, tokens), F32)],
        gram,
        received_gram,
        gained,
    )
    all_rows = encoded
    blocks = [0]
    for distance in reversed(distances(count)):
        with jax.named_scope(f"rows{distance}"):
            received = swapped(all_rows, "dp", distance)
        all_rows = jnp.concatenate([all_rows, received], axis=0)
        blocks = blocks + [i ^ distance for i in blocks]
    (score_part,) = call(
        score_kernel,
        [((2 * total_rows + 2 * rank, max(tokens, total_rows)), F32)],
        all_rows,
        gained,
        gain,
        up_ordered,
        low_up,
    )
    received_scores = swapped(score_part, "tensor")

    place = jnp.arange(total_rows, dtype=jnp.int32)
    row_blocks = jnp.repeat(jnp.array(blocks, jnp.int32), rows_local)
    row_ids = (row_blocks ^ position) * rows_local + place % rows_local
    chosen = (row_ids[:, None] == place[None, :]) * tenant[0][None, :]
    tenants = jnp.sum(chosen, axis=1)
    row_loss, adapter_part, spread, late = call(
        loss_kernel,
        [
            ((1, rows_local), F32),
            ((2 * rank, half_width), BF16),
            ((rows_local, half_width), F32),
            ((rank + 8, tokens), F32),
        ],
        score_part,
        received_scores,
        tenants[None, :],
        tenants[:, None],
        token_terms,
        all_rows,
        unit,
        own_outputs,
        other_outputs,
        gain,
        low,
        own_tokens,
    )

    sums = [adapter_part[:rank], adapter_part[rank:]]
    orders = (distances(count), distances(count)[1:] + [1])
    for stage in range(len(orders[0])):
        with jax.named_scope(f"sum{stage}"):
            received = [swapped(v, "dp", order[stage]) for v, order in zip(sums, orders)]
        sums = [v.astype(F32) + r.astype(F32) for v, r in zip(sums, received)]
        if stage < len(orders[0]) - 1:
            sums = [v.astype(BF16) for v in sums]
    up_gradient = own_first(sums[0])
    down_gradient = sums[1]

    other_spread = swapped(spread[:, columns:], "pipe")
    spreads = jnp.concatenate([spread[:, :columns], other_spread], axis=0)
    spread_near, spread_far = features(spreads, "late")
    spread_total = spread_near + swapped(spread_far, "tensor")
    if crossed:
        late = swapped(late, "pipe")
        down_matrix = pick(adapter_down_maps, other_picked)
    (handed,) = call(
        input_kernel,
        [((tokens, half_width), BF16)],
        late,
        spread_total,
        near_half,
        received_half,
        down_matrix,
    )
    if not crossed:
        members = range(lax.axis_size("pipe"))
        handed = lax.ppermute(handed, "pipe", [((i + 1) % len(members), i) for i in members])
    return (handed[None], up_gradient[None], down_gradient[None], row_loss)


def solution(mesh):
    return jax.shard_map(
        body,
        mesh=mesh,
        in_specs=(
            P("pipe", "dp", "tensor"),
            P("dp", "tensor"),
            P("tensor"),
            P(None, None, "tensor"),
            P(None, None, "tensor"),
            P("pipe", None),
            P("pipe"),
        ),
        out_specs=(
            P("pipe", "dp", "tensor"),
            P("pipe", None, "tensor"),
            P("pipe", None, "tensor"),
            P("pipe", "dp"),
        ),
        check_vma=False,
    )
```

```python
import functools

import jax
import jax.numpy as jnp
from jax import lax
from jax.experimental import pallas as pl
from jax.experimental.pallas import tpu as pltpu
from jax.sharding import PartitionSpec as P


MODEL_WIDTH = 3584
SEQ = 16

logit_divisor = 0.05
loss_scale = 256.0
adapter_scale = 0.5
epsilon = 1e-06

F32 = jnp.float32
BF16 = jnp.bfloat16
EXACT = lax.Precision.HIGHEST
LAST = (((1,), (1,)), ((), ()))
FIRST = (((0,), (0,)), ((), ()))

CHUNKS = 2


def swapped(block, axis, distance=1, members=None):
    devices = range(lax.axis_size(axis)) if members is None else members
    return lax.ppermute(block, axis, [(i, i ^ distance) for i in devices])


def dot(a, b, dims=(((1,), (0,)), ((), ())), precision=None):
    return lax.dot_general(a, b, dims, precision=precision, preferred_element_type=F32)


def iota(shape, dim):
    return lax.broadcasted_iota(jnp.int32, shape, dim)


def same_sequence(tokens):
    return (iota((tokens, tokens), 0) // SEQ == iota((tokens, tokens), 1) // SEQ).astype(F32)


def column_of(row):
    tokens = row.shape[1]
    eye = iota((tokens, tokens), 0) == iota((tokens, tokens), 1)
    return jnp.sum(jnp.where(eye, row, 0.0), axis=1, keepdims=True)


def spread_rows(rows_local, tokens):
    return (iota((rows_local, tokens), 0) == iota((rows_local, tokens), 1) // SEQ).astype(F32)


def picked_map(adapter_ref, maps_ref):
    picked = maps_ref[0]
    for i in range(1, maps_ref.shape[0]):
        picked = jnp.where(adapter_ref[...] == i, maps_ref[i], picked)
    return picked


def adapter_kernel(count, rows_local, adapter_ref, down_ref, up_ref, hidden_ref, gain_ref, tenant_ref, *outs):
    low_ref, down_out_ref, up_out_ref, gain_out_ref, allowed_ref = outs
    half = gain_ref.shape[1] // 2
    is_first = lax.axis_index("pipe") % 2 == 0
    down = picked_map(adapter_ref, down_ref)
    down_out_ref[...] = down
    low_ref[...] = dot(down, hidden_ref[...], LAST)
    up = picked_map(adapter_ref, up_ref)
    gain = jnp.broadcast_to(gain_ref[...], gain_out_ref.shape)
    for source, out_ref in ((up, up_out_ref), (gain, gain_out_ref)):
        lower, upper = source[:, :half], source[:, half:]
        out_ref[:, :half] = jnp.where(is_first, lower, upper)
        out_ref[:, half:] = jnp.where(is_first, upper, lower)
    total = tenant_ref.shape[1]
    row = iota((total, total), 1)
    slot = row // rows_local
    offset = jnp.zeros_like(slot)
    for i, distance in enumerate(reversed(distances(count))):
        offset = offset + ((slot >> i) & 1) * distance
    ids = (offset ^ lax.axis_index("dp")) * rows_local + row % rows_local
    tenants = column_of(tenant_ref[...].astype(F32))
    placed = jnp.sum(jnp.where(iota((total, total), 0) == ids, tenants, 0.0), axis=0, keepdims=True)
    allowed = (column_of(placed) == placed) & (iota((total, total), 0) != row)
    allowed_ref[...] = allowed.astype(F32)


def low_kernel(adapter_ref, down_ref, up_ref, own_up_ref, low_ref, other_low_ref, out_ref, down_out_ref):
    tokens = low_ref.shape[1]
    half = out_ref.shape[1]
    is_first = lax.axis_index("pipe") % 2 == 0
    down_out_ref[...] = picked_map(adapter_ref, down_ref)
    up = picked_map(adapter_ref, up_ref)
    other_up = jnp.where(is_first, up[:, :half], up[:, half:])
    out_ref[:tokens, :] = adapter_scale * dot(low_ref[...], own_up_ref[:, :half], FIRST)
    out_ref[tokens:, :] = adapter_scale * dot(other_low_ref[...], other_up, FIRST)


def gram_kernel(*refs):
    outputs_ref, gain_ref, up_ref = refs[:3]
    gram_ref, gained_ref, low_up_ref = refs[-3:]
    outputs = outputs_ref[...]
    tokens, half = outputs.shape
    gained = (outputs.reshape(tokens // 8, 8, half) * gain_ref[...][None]).reshape(tokens, half)
    gained_ref[...] = gained
    high = gained.astype(BF16)
    rest = (gained - high.astype(F32)).astype(BF16)
    cross = dot(high, rest, LAST) + dot(rest, high, LAST)
    gram = (dot(high, high, LAST) + cross) * same_sequence(tokens)
    fold = (iota((SEQ, tokens), 1) % SEQ == iota((SEQ, tokens), 0)).astype(F32)
    gram = dot(fold, gram, precision=EXACT)
    squares = outputs * outputs
    lanes = sum(squares[:, i : i + 128] for i in range(0, half, 128))
    squares = dot(jnp.ones((8, 128), F32), lanes, LAST, EXACT)
    low_up = dot(up_ref[...], outputs.astype(BF16), LAST)
    if len(refs) > 6:
        gram = gram + refs[3][0:SEQ, :]
        squares = squares + refs[3][SEQ : SEQ + 8, :]
        low_up = low_up + refs[4][...]
    gram_ref[0:SEQ, :] = gram
    gram_ref[SEQ : SEQ + 8, :] = squares
    low_up_ref[...] = low_up


def sum_kernel(up_ref, up_received_ref, down_ref, down_received_ref, up_out_ref, down_out_ref):
    half = up_ref.shape[1] // 2
    total = up_ref[...].astype(F32) + up_received_ref[...].astype(F32)
    own, other = total[:, :half], total[:, half:]
    is_first = lax.axis_index("pipe") % 2 == 0
    up_out_ref[:, :half] = jnp.where(is_first, own, other)
    up_out_ref[:, half:] = jnp.where(is_first, other, own)
    down_out_ref[...] = down_ref[...].astype(F32) + down_received_ref[...].astype(F32)


def pool_kernel(gram_ref, received_ref, own_ref, other_ref, unit_ref, encoded_ref, token_ref):
    tokens, half = own_ref.shape
    rows_local = tokens // SEQ
    total = gram_ref[...] + received_ref[...]
    token_inv = lax.rsqrt(total[SEQ : SEQ + 1, :] / MODEL_WIDTH + epsilon)
    same = same_sequence(tokens)
    place = (iota((SEQ, tokens), 1) % SEQ == iota((SEQ, tokens), 0)).astype(F32)
    peers = dot(place * token_inv, same, precision=EXACT)
    weighted = jnp.sum(total[0:SEQ, :] * peers, axis=0, keepdims=True)
    parts = jnp.broadcast_to(token_inv * weighted, (8, tokens))
    squares = dot(parts, same, precision=EXACT)[0:1, :] / (SEQ * SEQ)
    inverse = lax.rsqrt(squares + epsilon)
    pick = spread_rows(rows_local, tokens) * (token_inv * inverse / SEQ)
    for i, gained_ref in enumerate((own_ref, other_ref)):
        unit = dot(pick, gained_ref[...], precision=EXACT)
        unit_ref[:, i * half : (i + 1) * half] = unit
        encoded_ref[:, i * half : (i + 1) * half] = unit.astype(BF16)
    token_ref[0:1, :] = token_inv
    token_ref[1:2, :] = inverse
    token_ref[2:3, :] = inverse * weighted / SEQ
    token_ref[3:8, :] = jnp.zeros((5, tokens), F32)


def score_kernel(rows_ref, own_ref, other_ref, gain_ref, up_ref, low_up_ref, out_ref):
    total_rows = rows_ref.shape[0]
    rank, _ = low_up_ref.shape
    width = out_ref.shape[1]

    def put(start, value):
        rows, columns = value.shape
        if columns < width:
            value = jnp.concatenate([value, jnp.zeros((rows, width - columns), F32)], axis=1)
        out_ref[start : start + rows, :] = value

    rows = rows_ref[...]
    gained_rows = (rows.astype(F32) * gain_ref[0:1, :]).astype(BF16)
    put(0, dot(rows, rows, LAST))
    half = own_ref.shape[1]
    own = dot(rows[:, :half], own_ref[...].astype(BF16), LAST)
    put(total_rows, own + dot(rows[:, half:], other_ref[...].astype(BF16), LAST))
    put(2 * total_rows, low_up_ref[...])
    put(2 * total_rows + rank, dot(up_ref[...], gained_rows, LAST))


def loss_kernel(
    part_ref,
    received_ref,
    allowed_ref,
    token_ref,
    rows_ref,
    unit_ref,
    own_ref,
    other_ref,
    gain_ref,
    low_ref,
    hidden_ref,
    loss_ref,
    adapter_ref,
    spread_ref,
    late_ref,
):
    total_rows = rows_ref.shape[0]
    rows_local = unit_ref.shape[0]
    rank, tokens = low_ref.shape
    total = part_ref[...] + received_ref[...]
    products = total[0:total_rows, 0:total_rows]
    scores = products / logit_divisor
    from_row = iota((total_rows, total_rows), 0)
    from_column = iota((total_rows, total_rows), 1)
    allowed = allowed_ref[...] > 0.0
    partner = from_column == (from_row ^ 1)
    exps = jnp.where(allowed, jnp.exp(scores), 0.0)
    log_total = jnp.log(jnp.sum(exps, axis=1, keepdims=True))
    positive = jnp.sum(jnp.where(partner, scores, 0.0), axis=1, keepdims=True)
    own = (iota((total_rows, rows_local), 0) == iota((total_rows, rows_local), 1)).astype(F32)
    loss_ref[...] = jnp.sum((log_total - positive) * own, axis=0, keepdims=True)
    probs = jnp.where(allowed, jnp.exp(scores - log_total), 0.0)
    weights = loss_scale * (probs - partner.astype(F32))
    weights = weights.astype(BF16)
    near = weights[0:rows_local, :]
    far = dot(own.astype(BF16), weights, (((0,), (1,)), ((), ()))).astype(BF16)
    both = near.astype(F32) + far.astype(F32)
    rows = rows_ref[...]
    derivative = (dot(near, rows) + dot(far, rows)) / logit_divisor
    along = jnp.sum(both * products[0:rows_local, :], axis=1, keepdims=True) / logit_divisor
    expand = spread_rows(rows_local, tokens)
    along_row = jnp.sum(along * expand, axis=0, keepdims=True)
    token_weights = dot(both, expand, FIRST, EXACT)
    first = jnp.sum(token_weights * total[total_rows : 2 * total_rows, 0:tokens], axis=0, keepdims=True)
    first = first / logit_divisor
    token_inv = token_ref[0:1, :]
    inverse = token_ref[1:2, :]
    second = token_ref[2:3, :]
    inner = inverse * (first - along_row * second) / SEQ
    decay = token_inv * token_inv * token_inv * inner / MODEL_WIDTH
    inverse_column = jnp.sum(expand * inverse, axis=1, keepdims=True) / SEQ
    unit = unit_ref[...]
    spread = inverse_column * (derivative - unit * along) * gain_ref[0:1, :] / SEQ
    spread_ref[...] = spread
    inv_column = column_of(token_inv)
    decay_column = column_of(decay)
    half = own_ref.shape[1]
    width = 2 * half
    wide = jnp.broadcast_to(spread[:, None, :], (rows_local, SEQ, width)).reshape(tokens, width)
    outputs = jnp.concatenate([own_ref[...], other_ref[...]], axis=1)
    output_gradient = (inv_column * wide - decay_column * outputs).astype(BF16)
    adapter_ref[0:rank, :] = (adapter_scale * dot(low_ref[...], output_gradient)).astype(BF16)
    start = 2 * total_rows
    low_up = total[start : start + rank, 0:tokens]
    rows_up = total[start + rank : start + 2 * rank, 0:total_rows]
    sums_up = dot(rows_up, token_weights, precision=EXACT) / logit_divisor
    own_up = dot(rows_up[:, 0:rows_local], expand, precision=EXACT)
    spread_up = inverse * (sums_up - own_up * along_row) / SEQ
    low_gradient = (adapter_scale * (token_inv * spread_up - decay * low_up)).astype(BF16)
    adapter_ref[rank : 2 * rank, :] = dot(low_gradient, hidden_ref[...]).astype(BF16)
    late_ref[0:rank, :] = low_gradient.astype(F32)
    late_ref[rank : rank + 1, :] = token_inv
    late_ref[rank + 1 : rank + 2, :] = decay
    late_ref[rank + 2 : rank + 8, :] = jnp.zeros((6, tokens), F32)


def input_kernel(late_ref, spread_ref, part_ref, received_ref, down_ref, out_ref):
    tokens, width = part_ref.shape
    rank = down_ref.shape[0]
    rows_local = spread_ref.shape[0]
    inv_column = column_of(late_ref[rank : rank + 1, :])
    decay_column = column_of(late_ref[rank + 1 : rank + 2, :])
    low_gradient = late_ref[0:rank, :].astype(BF16)
    wide = jnp.broadcast_to(spread_ref[...][:, None, :], (rows_local, SEQ, width))
    total = part_ref[...] + received_ref[...].astype(F32)
    base = inv_column * wide.reshape(tokens, width) - decay_column * total
    out_ref[...] = (base + dot(low_gradient, down_ref[...], FIRST)).astype(BF16)


def call(kernel, outs, *args):
    vmem = pl.BlockSpec(memory_space=pltpu.VMEM)
    size = sum(a.size * a.dtype.itemsize for a in args)
    return pl.pallas_call(
        kernel,
        out_shape=[jax.ShapeDtypeStruct(shape, dtype) for shape, dtype in outs],
        in_specs=[vmem] * len(args),
        out_specs=[vmem] * len(outs),
        cost_estimate=pl.CostEstimate(flops=2**28, bytes_accessed=size, transcendentals=0),
        compiler_params=pltpu.CompilerParams(vmem_limit_bytes=12 * 2**20),
    )(*args)


def distances(count):
    return [2**i for i in range(count.bit_length() - 1)]


def gathered_blocks(own, is_inner, values, then):
    count = lax.axis_size("dp")
    if count != 8:
        block = own.shape[0]
        held = own
        for distance in distances(count):
            held = jnp.concatenate([held, swapped(held, "dp", distance)], axis=0)
        return [[held[i * block : (i + 1) * block]] for i in range(count)], then(values)
    inner = [i for i in range(count) if i // 2 in (1, 2)]
    outer = [i for i in range(count) if i // 2 in (0, 3)]
    forward = [(i ^ 2, i) for i in outer]
    rows = own.shape[0] // CHUNKS
    states = [dict(own=own[i * rows : (i + 1) * rows]) for i in range(CHUNKS)]
    results = []
    for step in range(4 * CHUNKS):
        chunk = step % CHUNKS
        state = states[chunk]
        if step >= 2:
            if step == 6:
                values = then(values)
            held = values if step in (4, 6) else ()
            tied, held = lax.optimization_barrier(({**state, **results[step - 2]}, held))
            values = held if step in (4, 6) else values
            state.update(tied)
        stage = step // CHUNKS
        new = {}
        if stage == 0:
            new["own_x"] = swapped(state["own"], "dp", 1)
            new["near"] = swapped(state["own"], "dp", 2)
            new["across"] = swapped(state["own"], "dp", 6, inner)
        elif stage == 1:
            new["near_x"] = swapped(state["near"], "dp", 1)
            new["across_second"] = swapped(state["near"], "dp", 6, inner)
            new["forward_first"] = lax.ppermute(state["across"], "dp", forward)
        elif stage == 2:
            second = jnp.where(is_inner, state["across_second"], state["forward_first"])
            state["second"] = lax.optimization_barrier(second)
            new["second_x"] = swapped(state["second"], "dp", 1)
            new["forward_second"] = lax.ppermute(state["across_second"], "dp", forward)
            if chunk > 0:
                new["across_x"] = swapped(state["own_x"], "dp", 6, inner)
        elif chunk == 0:
            third = jnp.where(is_inner, state["across"], state["forward_second"])
            state["third"] = lax.optimization_barrier(third)
            new["third_x"] = swapped(state["third"], "dp", 1)
        else:
            new["forward_x"] = lax.ppermute(state["second_x"], "dp", forward)
        state.update(new)
        results.append(new)
    names = ("own", "own_x", "near", "near_x", "second", "second_x")
    slots = [[state[name] for state in states] for name in names]
    first, last = states
    slots.append([first["third"], last["across"], last["forward_second"]])
    slots.append([first["third_x"], last["across_x"], last["forward_x"]])
    return slots, values


def forward_kernel(first, *refs):
    own_ref, other_ref, start_ref = refs[:3]
    outs = refs[-2:] if first else refs[-4:]
    pieces = refs[3 : -len(outs)]
    total_ref, weight_ref = outs[0], outs[-1]
    position = lax.axis_index("dp")
    is_inner = (((position >> 1) + 1) & 2) != 0
    each = CHUNKS if first else 3
    rows = pieces[0].shape[0]
    block = rows * CHUNKS
    tokens = own_ref.shape[0]
    total = start_ref[...]
    offset = 0 if first else own_ref.shape[1] // (2 * block) - 1
    for pair in range(len(pieces) // (2 * each)):
        for i in range(2):
            parts = [ref[...] for ref in pieces[(2 * pair + i) * each : (2 * pair + i + 1) * each]]
            if not first:
                parts = [parts[0], jnp.where(is_inner, parts[1], parts[2])]
            where = pair * 2 * block + ((position & 1) ^ i) * block
            for j, part in enumerate(parts):
                weight_ref[pl.ds(pl.multiple_of(where + j * rows, 16), rows), :] = part
        lane = pl.ds(pl.multiple_of(((position >> 1) ^ (pair + offset)) * 2 * block, 128), 2 * block)
        x = jnp.concatenate([own_ref[:, lane], other_ref[:, lane]], axis=0)
        total = total + dot(x, weight_ref[pair * 2 * block : (pair + 1) * 2 * block, :])
    if first:
        total_ref[...] = total
    else:
        total_ref[...] = total[:tokens]
        outs[1][...] = total[tokens:]
        outs[2][...] = total.astype(BF16)


def product_kernel(rows_ref, low_ref, high_ref, near_ref, far_ref):
    size = rows_ref.shape[1]
    rows = rows_ref[...].astype(BF16)
    position = lax.axis_index("dp")
    bit = (position >> 1) & 1
    for i in range(2):
        weight = low_ref[pl.ds(pl.multiple_of((bit ^ i) * size, 128), size), :]
        same = dot(rows, weight, LAST)
        weight = jnp.where(bit == i, low_ref[2 * size : 3 * size, :], high_ref[...])
        other = dot(rows, weight, LAST)
        stays = (position >> 2) == lax.axis_index("tensor")
        near_ref[:, i * size : (i + 1) * size] = jnp.where(stays, same, other)
        far_ref[:, i * size : (i + 1) * size] = jnp.where(stays, other, same)


def body(
    hidden, frozen_weight, final_norm_gain, adapter_down_maps, adapter_up_maps, tenant, adapter
):
    own_tokens = hidden[0]
    tokens, half_width = own_tokens.shape
    rows_local = tokens // SEQ
    columns = half_width // 2
    rank = adapter_up_maps.shape[1]
    count = lax.axis_size("dp")
    position = lax.axis_index("dp")
    side = lax.axis_index("tensor")
    core = lax.axis_index("pipe") & 1
    crossed = lax.axis_size("pipe") == 2
    total_rows = count * rows_local

    weight_part = lax.dynamic_slice_in_dim(frozen_weight, core * columns, columns, axis=1)
    flags = ((((position >> 1) + 1) & 2) != 0, side == 0)
    weight_part, (is_inner, is_left) = lax.optimization_barrier((weight_part, flags))
    low_part, down_matrix, up_ordered, gain, allowed = call(
        functools.partial(adapter_kernel, count, rows_local),
        [
            ((rank, tokens), F32),
            ((rank, half_width), BF16),
            ((rank, half_width), BF16),
            ((8, half_width), F32),
            ((total_rows, total_rows), F32),
        ],
        adapter[None, :],
        adapter_down_maps,
        adapter_up_maps,
        own_tokens,
        final_norm_gain[None, :],
        tenant,
    )
    values = (
        swapped(own_tokens, "tensor"),
        swapped(low_part, "tensor"),
        swapped(adapter, "pipe")[None, :],
        low_part,
        up_ordered,
    )

    def then(values):
        received_tokens, received_low, other_adapter, low_part, up_ordered = values
        full_tokens = jnp.where(
            is_left,
            jnp.concatenate([own_tokens, received_tokens], axis=1),
            jnp.concatenate([received_tokens, own_tokens], axis=1),
        )
        low = (low_part + received_low).astype(BF16)
        low_outputs, other_down = call(
            low_kernel,
            [((2 * tokens, columns), F32), ((rank, half_width), BF16)],
            other_adapter,
            adapter_down_maps,
            adapter_up_maps,
            up_ordered,
            low,
            swapped(low, "pipe"),
        )
        return full_tokens, swapped(full_tokens, "pipe"), low, low_outputs, other_down

    slots, values = gathered_blocks(weight_part, is_inner, values, then)
    full_tokens, other_tokens, low, low_outputs, other_down = values

    in_pairs = len(slots[-1]) == 3
    if in_pairs:
        early = [piece for slot in slots[:6] for piece in slot]
        last = [piece for slot in slots[6:] for piece in slot]
        pair_rows = 2 * weight_part.shape[0]
        partial_outputs, weight_low = call(
            functools.partial(forward_kernel, True),
            [((2 * tokens, columns), F32), ((3 * pair_rows, columns), BF16)],
            full_tokens,
            other_tokens,
            low_outputs,
            *early,
        )
        own_outputs, sent_outputs, outputs_low, weight_high = call(
            functools.partial(forward_kernel, False),
            [
                ((tokens, columns), F32),
                ((tokens, columns), F32),
                ((2 * tokens, columns), BF16),
                ((pair_rows, columns), BF16),
            ],
            full_tokens,
            other_tokens,
            partial_outputs,
            *last,
        )
    else:
        weight = jnp.zeros((count * weight_part.shape[0], columns), BF16)
        for i, (piece,) in enumerate(slots):
            start = (position ^ i) * weight_part.shape[0]
            weight = lax.dynamic_update_slice(weight, piece, (start, 0))
        both_tokens = jnp.concatenate([full_tokens, other_tokens], axis=0)
        outputs = dot(both_tokens, weight) + low_outputs
        own_outputs, sent_outputs = outputs[:tokens], outputs[tokens:]
        outputs_low = outputs.astype(BF16)

    def features(rows):
        if in_pairs:
            shape = (rows.shape[0], half_width)
            products = call(
                product_kernel, [(shape, F32)] * 2, rows, weight_low, weight_high
            )
        else:
            product = dot(rows.astype(BF16), weight, LAST)
            lower, upper = product[:, :half_width], product[:, half_width:]
            products = (jnp.where(side == 0, lower, upper), jnp.where(side == 0, upper, lower))
        sums = []
        half = rows.shape[0] // 2
        for product in products:
            kept, sent = (product[half:], product[:half])
            if not crossed:
                kept, sent = sent, kept
            if half == tokens:
                sent = sent.astype(BF16)
            sums.append(kept + swapped(sent, "pipe").astype(F32))
        return sums

    other_outputs = swapped(sent_outputs, "pipe")

    near_half, far_half = features(outputs_low)
    received_half = swapped(far_half.astype(BF16), "tensor")

    gram_outs = [((SEQ + 8, tokens), F32), ((tokens, columns), F32), ((rank, tokens), F32)]
    gram, own_gained, low_up = call(
        gram_kernel, gram_outs, own_outputs, gain[:, :columns], up_ordered[:, :columns]
    )
    gram, other_gained, low_up = call(
        gram_kernel,
        gram_outs,
        other_outputs,
        gain[:, columns:],
        up_ordered[:, columns:],
        gram,
        low_up,
    )
    received_gram = swapped(gram, "tensor")
    unit, encoded, token_terms = call(
        pool_kernel,
        [((rows_local, half_width), F32), ((rows_local, half_width), BF16), ((8, tokens), F32)],
        gram,
        received_gram,
        own_gained,
        other_gained,
    )
    all_rows = encoded
    for distance in reversed(distances(count)):
        received = swapped(all_rows, "dp", distance)
        all_rows = jnp.concatenate([all_rows, received], axis=0)
    (score_part,) = call(
        score_kernel,
        [((2 * total_rows + 2 * rank, max(tokens, total_rows)), F32)],
        all_rows,
        own_gained,
        other_gained,
        gain,
        up_ordered,
        low_up,
    )
    received_scores = swapped(score_part, "tensor")

    row_loss, adapter_part, spread, late = call(
        loss_kernel,
        [
            ((1, rows_local), F32),
            ((2 * rank, half_width), BF16),
            ((rows_local, half_width), F32),
            ((rank + 8, tokens), F32),
        ],
        score_part,
        received_scores,
        allowed,
        token_terms,
        all_rows,
        unit,
        own_outputs,
        other_outputs,
        gain,
        low,
        own_tokens,
    )

    sums = [adapter_part[:rank], adapter_part[rank:]]
    orders = (distances(count), distances(count)[-1:] + distances(count)[:-1])
    for stage in range(len(orders[0])):
        received = [swapped(v, "dp", order[stage]) for v, order in zip(sums, orders)]
        if stage < len(orders[0]) - 1:
            sums = [(v.astype(F32) + r.astype(F32)).astype(BF16) for v, r in zip(sums, received)]
    up_gradient, down_gradient = call(
        sum_kernel,
        [((rank, half_width), F32)] * 2,
        sums[0],
        received[0],
        sums[1],
        received[1],
    )

    other_spread = swapped(spread[:, columns:], "pipe")
    spreads = jnp.concatenate([spread[:, :columns], other_spread], axis=0)
    spread_near, spread_far = features(spreads)
    spread_total = spread_near + swapped(spread_far, "tensor")
    if crossed:
        late = swapped(late, "pipe")
        down_matrix = other_down
    (handed,) = call(
        input_kernel,
        [((tokens, half_width), BF16)],
        late,
        spread_total,
        near_half,
        received_half,
        down_matrix,
    )
    if not crossed:
        members = range(lax.axis_size("pipe"))
        handed = lax.ppermute(handed, "pipe", [((i + 1) % len(members), i) for i in members])
    return (handed[None], up_gradient[None], down_gradient[None], row_loss)


def solution(mesh):
    return jax.shard_map(
        body,
        mesh=mesh,
        in_specs=(
            P("pipe", "dp", "tensor"),
            P("dp", "tensor"),
            P("tensor"),
            P(None, None, "tensor"),
            P(None, None, "tensor"),
            P("pipe", None),
            P("pipe"),
        ),
        out_specs=(
            P("pipe", "dp", "tensor"),
            P("pipe", None, "tensor"),
            P("pipe", None, "tensor"),
            P("pipe", "dp"),
        ),
        check_vma=False,
    )
```
